128 devices in a mesh: zs: 8 (over z, core), ys: 16 (over y, x).
Axes of the slice: x: 4, y: 4, z: 4, core: 2. Of those that a mesh axis runs over, the one named last changes fastest.
Arguments:
- polarization: bfloat16 [2, 6, 256, 256, 1024], P(None, None, None, 'ys', 'zs'), may hold values from -6 to 6
- theta_index: int32 [512], replicated, may hold values from 0 to 179
- phi_index: int32 [512], replicated, may hold values from 0 to 359
Outputs:
- mueller: float32 [16, 512], replicated
The draws below stay inside these ranges and needn't reach their ends.
All inputs are finite; a program needn't handle non-finite values.
Results may differ from the reference program's by a relative error of at most 0.0033.
Values sent between devices are 32-bit elements.
No kernel may reach another device: no remote copies, remote signals or barrier semaphores. Data moves between devices by JAX's collectives and lax.ppermute only.
A program may use at most 64 MiB of HBM per device.

```python
import math
import jax
import jax.numpy as jnp
from jax import lax

GX = 256
DIRS = 512
NTHETA = 180
NPHI = 360
NY = 256
NZ = 1024


def with_ends(result, rng, least, largest):
    place = [jax.random.randint(jax.random.fold_in(rng, axis), (), 0, length) for axis, length in enumerate(result.shape)]
    longest = result.shape.index(max(result.shape))
    beside = place[:longest] + [(place[longest] + 1) % result.shape[longest]] + place[longest + 1:]
    return result.at[tuple(place)].set(least).at[tuple(beside)].set(largest)


def block_scale(rng, dims, split, smallest, high):
    def one(axis_at, shards_of):
        heights = jax.random.uniform(jax.random.fold_in(jax.random.fold_in(rng, 6), axis_at), (shards_of,), jnp.float32, smallest / len(split), high / len(split))
        return jnp.repeat(jnp.exp(heights), dims[axis_at] // shards_of).reshape((-1,) + (1,) * (len(dims) - axis_at - 1))

    gain = one(*split[0])
    for cut in split[1:]:
        gain = gain * one(*cut)
    return gain


def centred(own_key, dims, spread, limit, cuts=(), dtype=jnp.bfloat16):
    result = jax.random.normal(own_key, dims, jnp.float32) * spread
    if len(cuts) > 0:
        result = block_scale(own_key, dims, cuts, -0.22, 0.18) * result
    return jnp.clip(result, min=-limit, max=limit).astype(dtype)


def setup_inputs(seed: int = 0) -> dict:
    key_list = jax.random.split(jax.random.key(seed), 4)
    return {
        "polarization": centred(key_list[0], (2, 6, GX, NY, NZ), 1.0, 6.0, ((3, 16), (4, 8))),
        "theta_index": with_ends(jax.random.randint(key_list[1], (DIRS,), 0, NTHETA), jax.random.fold_in(key_list[1], 1), 0, NTHETA - 1).astype(jnp.int32),
        "phi_index": with_ends(jax.random.randint(key_list[2], (DIRS,), 0, NPHI), jax.random.fold_in(key_list[2], 1), 0, NPHI - 1).astype(jnp.int32),
    }


wave_step = 0.6
pauli_set = (((1, 0), (0, 1)), ((1, 0), (0, -1)), ((0, 1), (1, 0)), ((0, -1j), (1j, 0)))

def angles(theta_index, phi_index):
    polar_angle = math.pi * (theta_index.astype(jnp.float32) + 0.5) / NTHETA
    azimuth = 2.0 * math.pi * phi_index.astype(jnp.float32) / NPHI
    return (polar_angle, azimuth)

def mueller_of(amplitude, polar_angle, azimuth):
    unit_theta = (jnp.cos(polar_angle) * jnp.cos(azimuth), jnp.cos(polar_angle) * jnp.sin(azimuth), -jnp.sin(polar_angle))
    unit_phi = (-jnp.sin(azimuth), jnp.cos(azimuth))
    real_jones = [[None, None], [None, None]]
    imag_jones = [[None, None], [None, None]]
    for s, unit_vec in enumerate((unit_theta, unit_phi)):
        for p in range(2):
            real_sum = 0.0
            imag_sum = 0.0
            for c in range(len(unit_vec)):
                real_sum = real_sum + unit_vec[c] * amplitude[:, 3 * p + c]
                imag_sum = imag_sum + unit_vec[c] * amplitude[:, 6 + 3 * p + c]
            real_jones[s][p] = real_sum
            imag_jones[s][p] = imag_sum
    elements = []
    for i in range(4):
        for j in range(4):
            summed = 0.0
            for a in range(2):
                for b in range(2):
                    for c in range(2):
                        for e in range(2):
                            weight = complex(pauli_set[i][a][b]) * complex(pauli_set[j][c][e])
                            if weight == 0:
                                continue
                            z_real = real_jones[b][c] * real_jones[a][e] + imag_jones[b][c] * imag_jones[a][e]
                            z_imag = imag_jones[b][c] * real_jones[a][e] - real_jones[b][c] * imag_jones[a][e]
                            summed = summed + weight.real * z_real - weight.imag * z_imag
            elements.append(0.5 * summed)
    return jnp.stack(elements)

def reference(polarization, theta_index, phi_index):
    halves, components, cells_x, total_y, total_z = polarization.shape
    polar_angle, azimuth = angles(theta_index, phi_index)
    unit_x = jnp.sin(polar_angle) * jnp.cos(azimuth)
    unit_y = jnp.sin(polar_angle) * jnp.sin(azimuth)
    unit_z = jnp.cos(polar_angle)
    pos_x = (jnp.arange(cells_x) - cells_x // 2).astype(jnp.float32)
    pos_y = (jnp.arange(total_y) - total_y // 2).astype(jnp.float32)
    pos_z = (jnp.arange(total_z) - total_z // 2).astype(jnp.float32)
    flattened = polarization.astype(jnp.float32).reshape(halves, components, cells_x, total_y * total_z)
    scaling = 1.0 / math.sqrt(cells_x * total_y * total_z)
    block_size = 8

    def one_block(first_row):
        bx = lax.dynamic_slice_in_dim(unit_x, first_row, block_size)
        by = lax.dynamic_slice_in_dim(unit_y, first_row, block_size)
        bz = lax.dynamic_slice_in_dim(unit_z, first_row, block_size)
        phase_x = wave_step * bx[:, None] * pos_x[None, :]
        tables = jnp.stack([jnp.cos(phase_x), jnp.sin(phase_x)]).astype(jnp.bfloat16)
        summed = jnp.einsum('tdx,rcxq->tdrcq', tables.astype(jnp.float32), flattened, precision=lax.Precision.HIGHEST)
        real_x = summed[0, :, 0] + summed[1, :, 1]
        imag_x = summed[0, :, 1] - summed[1, :, 0]
        phase_yz = wave_step * (by[:, None, None] * pos_y[None, :, None] + bz[:, None, None] * pos_z[None, None, :])
        phase_yz = phase_yz.reshape(block_size, total_y * total_z)
        cos_yz = jnp.cos(phase_yz)[:, None, :]
        sin_yz = jnp.sin(phase_yz)[:, None, :]
        real_part = lax.optimization_barrier(jnp.sum(real_x * cos_yz + imag_x * sin_yz, axis=-1))
        imag_part = lax.optimization_barrier(jnp.sum(imag_x * cos_yz - real_x * sin_yz, axis=-1))
        return jnp.concatenate([real_part, imag_part], axis=1) * scaling
    firsts = (jnp.arange(DIRS // block_size) * block_size).astype(jnp.int32)
    amplitude = lax.map(one_block, firsts).reshape(DIRS, 12)
    return mueller_of(amplitude, polar_angle, azimuth)
```

```python
import functools, math
import jax, jax.numpy as jnp
from jax import lax
from jax.experimental import pallas as pl
from jax.experimental.pallas import tpu as pltpu
from jax.sharding import PartitionSpec as P

WAVE = 0.6
XB = 16
ORIENT = 2
AXES = True

def sincos_turns(u):
    r = u - jnp.floor(u + 0.5)
    t = r * r
    w = 2.0 * math.pi
    cos_k = [(-1) ** n * w ** (2 * n) / math.factorial(2 * n) for n in range(11)]
    sin_k = [(-1) ** n * w ** (2 * n + 1) / math.factorial(2 * n + 1) for n in range(10)]
    c = jnp.full_like(t, cos_k[-1])
    for k in cos_k[-2::-1]:
        c = c * t + k
    s = jnp.full_like(t, sin_k[-1])
    for k in sin_k[-2::-1]:
        s = s * t + k
    return c, s * r

def kernel(th_ref, ph_ref, p_hbm, out_ref, pv, w_ref, t_ref, acc_ref, tc_ref, ts_ref, sems):
    _, _, gx, ny, nz = pv.shape
    half = gx // 2
    dirs = th_ref.shape[1]
    f32, bf16 = jnp.float32, jnp.bfloat16
    nfold = half // XB - 1
    kb = XB * ny
    pieces = []
    for i in range(nfold):
        pieces.append([(half + 1 + XB * i, XB), (half - XB * (i + 1), XB)])
    pieces.append([(half, 1), (gx - XB + 1, XB - 1)])
    pieces.append([(0, XB)])
    copies = []
    n = 0
    for group in pieces:
        made = []
        for x0, cnt in group:
            made.append(pltpu.make_async_copy(p_hbm.at[:, :, pl.ds(x0, cnt)], pv.at[:, :, pl.ds(x0, cnt)], sems.at[n]))
            n += 1
        copies.append(made)
    ahead = 4
    for made in copies[:ahead]:
        for cp in made: cp.start()

    ct, st = sincos_turns((th_ref[...].astype(f32) + 0.5) * (1.0 / 360.0))
    cp_, sp_ = sincos_turns(ph_ref[...].astype(f32) * (1.0 / 360.0))
    scale = WAVE / (2.0 * math.pi)
    ux, uy, uz = scale * (st * cp_), scale * (st * sp_), scale * ct
    rows = tc_ref.shape[0]
    px = lax.broadcasted_iota(jnp.int32, (rows, dirs), 0).astype(f32)
    c, s = sincos_turns(px * ux)
    tc_ref[...] = c.astype(bf16).astype(f32)
    ts_ref[...] = s.astype(bf16).astype(f32)
    qy = lax.broadcasted_iota(jnp.int32, (ny, dirs), 0).astype(f32) - (ny - 1) / 2.0
    cy, sy = sincos_turns(qy * uy)
    flip_idx = 7 - lax.broadcasted_iota(jnp.int32, (2, 6, ny // 8, 8, nz), 3)

    def make_tables(step, slot):
        for xl in range(XB):
            if step < nfold: px = 1 + XB * step + xl
            elif step == nfold: px = 0 if xl == 0 else half - XB + xl
            else: px = xl - half
            tc = tc_ref[pl.ds(abs(px), 1), :]
            ts = ts_ref[pl.ds(abs(px), 1), :]
            if px < 0: ts = -ts
            k = xl * ny
            t_ref[slot, pl.ds(k, ny), :] = (tc * cy - ts * sy).astype(bf16)
            t_ref[slot, pl.ds(kb + k, ny), :] = (ts * cy + tc * sy).astype(bf16)

    def fill(step, slot):
        for xl in range(XB):
            k = xl * ny
            if step < nfold:
                off = 1 + XB * step + xl
                p = pv[:, :, half + off]
                m = pv[:, :, half - off].astype(f32).reshape(2, 6, ny // 8, 8, nz)
                m = jnp.take_along_axis(m, flip_idx, axis=3)
                m = jnp.concatenate([m[:, :, 1:2], m[:, :, 0:1]], axis=2).reshape(2, 6, ny, nz).astype(bf16)
                e = p + m
                er, ei = e[0], e[1]
                oi = p[1] - m[1]
                nor = m[0] - p[0]
            else:
                x = (half if xl == 0 else gx - XB + xl) if step == nfold else xl
                p = pv[:, :, x]
                er, ei, oi, nor = p[0], p[1], p[1], -p[0]
            w_ref[slot, 0:6, pl.ds(k, ny), :] = er
            w_ref[slot, 6:12, pl.ds(k, ny), :] = ei
            w_ref[slot, 0:6, pl.ds(kb + k, ny), :] = oi
            w_ref[slot, 6:12, pl.ds(kb + k, ny), :] = nor

    def multiply(step, slot):
        w = jnp.concatenate([w_ref[slot, j] for j in range(12)], axis=1)
        t = t_ref[slot]
        if ORIENT == 2:
            g = lax.dot_general(w, t, (((0,), (0,)), ((), ())), preferred_element_type=f32)
        else:
            g = lax.dot_general(t, w, (((0,), (0,)), ((), ())), preferred_element_type=f32)
        if step == 0: acc_ref[...] = g
        else: acc_ref[...] += g

    steps = len(copies)
    make_tables(0, 0)
    for cp in copies[0]: cp.wait()
    fill(0, 0)
    for step in range(steps):
        if step + ahead < steps:
            for cp in copies[step + ahead]: cp.start()
        if step + 1 < steps:
            for cp in copies[step + 1]: cp.wait()
            make_tables(step + 1, (step + 1) % 2)
            fill(step + 1, (step + 1) % 2)
        multiply(step, step % 2)

    if AXES:
        ys, total_y = lax.axis_index("ys"), ny * lax.axis_size("ys")
        zs, total_z = lax.axis_index("zs"), nz * lax.axis_size("zs")
    else:
        ys, total_y, zs, total_z = 3, 256, 2, 1024
    cyg = jnp.float32(ys * ny - total_y // 2) + (ny - 1) / 2.0
    z0 = jnp.float32(zs * nz - total_z // 2)
    qz = lax.broadcasted_iota(jnp.int32, (nz, dirs), 0).astype(f32) + z0
    cz, sz = sincos_turns(qz * uz + cyg * uy)
    total = 1.0 / math.sqrt(gx * total_y * total_z)
    outs = [None] * 12
    for c in range(6):
        if ORIENT == 2:
            re = acc_ref[pl.ds(c * nz, nz), :]
            im = acc_ref[pl.ds((6 + c) * nz, nz), :]
            outs[c] = jnp.sum(re * cz + im * sz, axis=0, keepdims=True) * total
            outs[6 + c] = jnp.sum(im * cz - re * sz, axis=0, keepdims=True) * total
    result = jnp.concatenate(outs, axis=0)
    for i in range(out_ref.shape[0]):
        out_ref[i] = result

def far_field(p, th, ph, copies):
    dirs = th.shape[1]
    r, ncomp, gx, ny, nz = p.shape
    return pl.pallas_call(
        kernel,
        name="far_field",
        out_shape=jax.ShapeDtypeStruct((copies, 12, dirs), jnp.float32),
        in_specs=[pl.BlockSpec(memory_space=pltpu.VMEM),
                  pl.BlockSpec(memory_space=pltpu.VMEM), pl.BlockSpec(memory_space=pl.ANY)],
        out_specs=pl.BlockSpec(memory_space=pltpu.VMEM),
        scratch_shapes=[
            pltpu.VMEM((r, ncomp, gx, ny, nz), jnp.bfloat16),
            pltpu.VMEM((2, 12, 2 * XB * ny, nz), jnp.bfloat16),
            pltpu.VMEM((2, 2 * XB * ny, dirs), jnp.bfloat16),
            pltpu.VMEM((12 * nz, dirs), jnp.float32),
            pltpu.VMEM((gx // 2 + 8, dirs), jnp.float32),
            pltpu.VMEM((gx // 2 + 8, dirs), jnp.float32),
            pltpu.SemaphoreType.DMA((2 * (gx // 2 // XB) + 1,)),
        ],
        compiler_params=pltpu.CompilerParams(vmem_limit_bytes=50 * 2**20),
    )(th, ph, p)


def sum_kernel(x_ref, o_ref):
    total = x_ref[0]
    for i in range(1, x_ref.shape[0]):
        total = total + x_ref[i]
    for i in range(o_ref.shape[0]):
        o_ref[i] = total


def sum_copies(x, copies):
    return pl.pallas_call(
        sum_kernel,
        name="sum_copies",
        out_shape=jax.ShapeDtypeStruct((copies, *x.shape[1:]), jnp.float32),
    )(x)


PAULI = (((1, 0), (0, 1)), ((1, 0), (0, -1)), ((0, 1), (1, 0)), ((0, -1j), (1j, 0)))


def mueller_kernel(x_ref, th_ref, ph_ref, o_ref):
    amplitude = x_ref[0]
    for i in range(1, x_ref.shape[0]):
        amplitude = amplitude + x_ref[i]
    ct, st = sincos_turns((th_ref[...].astype(jnp.float32) + 0.5) * (1.0 / 360.0))
    cp, sp = sincos_turns(ph_ref[...].astype(jnp.float32) * (1.0 / 360.0))
    units = ((ct * cp, ct * sp, -st), (-sp, cp))
    re = [[None, None], [None, None]]
    im = [[None, None], [None, None]]
    for s, unit in enumerate(units):
        for p in range(2):
            a = b = 0.0
            for c, u in enumerate(unit):
                a = a + u * amplitude[3 * p + c : 3 * p + c + 1]
                b = b + u * amplitude[6 + 3 * p + c : 7 + 3 * p + c]
            re[s][p], im[s][p] = a, b
    known = {}

    def product(b, c, a, e):
        if (b, c, a, e) not in known:
            known[b, c, a, e] = (re[b][c] * re[a][e] + im[b][c] * im[a][e],
                                 im[b][c] * re[a][e] - re[b][c] * im[a][e])
        return known[b, c, a, e]

    for i in range(4):
        for j in range(4):
            total = 0.0
            for a in range(2):
                for b in range(2):
                    for c in range(2):
                        for e in range(2):
                            weight = complex(PAULI[i][a][b]) * complex(PAULI[j][c][e])
                            if weight == 0:
                                continue
                            zr, zi = product(b, c, a, e)
                            if weight.real:
                                total = total + weight.real * zr
                            if weight.imag:
                                total = total - weight.imag * zi
            o_ref[4 * i + j : 4 * i + j + 1, :] = 0.5 * total


def mueller(x, th, ph):
    return pl.pallas_call(
        mueller_kernel,
        name="mueller",
        out_shape=jax.ShapeDtypeStruct((16, x.shape[2]), jnp.float32),
    )(x, th, ph)


def body(polarization, theta_index, phi_index):
    dirs = theta_index.shape[0]
    th, ph = theta_index.reshape(1, dirs), phi_index.reshape(1, dirs)
    copies = far_field(polarization, th, ph, lax.axis_size("zs"))
    copies = lax.all_to_all(copies, "zs", split_axis=0, concat_axis=0, tiled=True)
    copies = sum_copies(copies, lax.axis_size("ys"))
    copies = lax.all_to_all(copies, "ys", split_axis=0, concat_axis=0, tiled=True)
    return mueller(copies, th, ph)


def solution(mesh):
    return jax.shard_map(
        body,
        mesh=mesh,
        in_specs=(P(None, None, None, "ys", "zs"), P(), P()),
        out_specs=P(),
        check_vma=False,
    )
```

```python
import math

import jax
import jax.numpy as jnp
from jax import lax
from jax.experimental import pallas as pl
from jax.experimental.pallas import tpu as pltpu
from jax.sharding import PartitionSpec as P

WAVE = 0.6
NTHETA = 180
NPHI = 360
XB = 16
GROUPS = (1, 2, 3, 3)
AHEAD = 9


def sincos_turns(u):
    r = u - jnp.floor(u + 0.5)
    t = r * r
    w = 2.0 * math.pi
    cos_k = [(-1) ** n * w ** (2 * n) / math.factorial(2 * n) for n in range(11)]
    sin_k = [(-1) ** n * w ** (2 * n + 1) / math.factorial(2 * n + 1) for n in range(10)]
    c = jnp.full_like(t, cos_k[-1])
    for k in cos_k[-2::-1]:
        c = c * t + k
    s = jnp.full_like(t, sin_k[-1])
    for k in sin_k[-2::-1]:
        s = s * t + k
    return c, s * r


def far_field_kernel(
    th_hbm, ph_hbm, p_hbm, out_ref, unit_ref,
    th_ref, ph_ref, pv, wr, wi, t_ref, acc_ref, tc_ref, ts_ref, cz_ref, sz_ref, idx_sems, sems,
):
    _, comps, gx, ny, nz = pv.shape
    half = gx // 2
    dirs = out_ref.shape[1]
    f32, bf16 = jnp.float32, jnp.bfloat16
    folded = half // XB - 1
    kb = XB * ny

    idx_copies = [
        pltpu.make_async_copy(th_hbm, th_ref, idx_sems.at[0]),
        pltpu.make_async_copy(ph_hbm, ph_ref, idx_sems.at[1]),
    ]
    for cp in idx_copies:
        cp.start()
    pieces = [[(half + 1 + XB * i, XB), (half - XB * (i + 1), XB)] for i in range(folded)]
    pieces += [[(half, 1), (gx - XB + 1, XB - 1)], [(0, XB)]]
    copies = []
    count = 0
    for group in pieces:
        made = []
        for x0, length in group:
            window = pl.ds(x0, length)
            made.append(pltpu.make_async_copy(p_hbm.at[:, :, window], pv.at[:, :, window], sems.at[count]))
            count += 1
        copies.append(made)
    chunks = len(copies)
    for made in copies[:AHEAD]:
        for cp in made:
            cp.start()

    for cp in idx_copies:
        cp.wait()
    ct, st = sincos_turns((th_ref[...].reshape(1, dirs).astype(f32) + 0.5) * (0.5 / NTHETA))
    cp_, sp_ = sincos_turns(ph_ref[...].reshape(1, dirs).astype(f32) * (1.0 / NPHI))
    unit_ref[...] = jnp.concatenate([ct, st, cp_, sp_], axis=0)
    scale = WAVE / (2.0 * math.pi)
    ux, uy, uz = scale * (st * cp_), scale * (st * sp_), scale * ct
    px = lax.broadcasted_iota(jnp.int32, tc_ref.shape, 0).astype(f32)
    c, s = sincos_turns(px * ux)
    tc_ref[...] = c.astype(bf16).astype(f32)
    ts_ref[...] = s.astype(bf16).astype(f32)
    qy = lax.broadcasted_iota(jnp.int32, (ny, dirs), 0).astype(f32) - (ny - 1) / 2.0
    cy, sy = sincos_turns(qy * uy)
    flip = 7 - lax.broadcasted_iota(jnp.int32, (2, comps, ny // 8, 8, nz), 3)

    def z_phases():
        ys, total_y = lax.axis_index("ys"), ny * lax.axis_size("ys")
        zs, total_z = lax.axis_index("zs"), nz * lax.axis_size("zs")
        y_mid = (ys * ny - total_y // 2).astype(f32) + (ny - 1) / 2.0
        z_first = (zs * nz - total_z // 2).astype(f32)
        qz = lax.broadcasted_iota(jnp.int32, (nz, dirs), 0).astype(f32) + z_first
        total = 1.0 / math.sqrt(gx * total_y * total_z)
        c, s = sincos_turns(qz * uz + y_mid * uy)
        cz_ref[...] = c * total
        sz_ref[...] = s * total

    def make_tables(chunk, slot, k0):
        for xl in range(XB):
            if chunk < folded:
                px = 1 + XB * chunk + xl
            elif chunk == folded:
                px = 0 if xl == 0 else half - XB + xl
            else:
                px = xl - half
            tc = tc_ref[pl.ds(abs(px), 1), :]
            ts = ts_ref[pl.ds(abs(px), 1), :]
            if px < 0:
                ts = -ts
            k = k0 + xl * ny
            t_ref[slot, pl.ds(k, ny), :] = (tc * cy - ts * sy).astype(bf16)
            t_ref[slot, pl.ds(kb + k, ny), :] = (ts * cy + tc * sy).astype(bf16)

    def fill(chunk, slot, k0):
        for xl in range(XB):
            k = k0 + xl * ny
            if chunk < folded:
                off = 1 + XB * chunk + xl
                p = pv[:, :, half + off].astype(f32)
                m = pv[:, :, half - off].astype(f32).reshape(2, comps, ny // 8, 8, nz)
                m = jnp.take_along_axis(m, flip, axis=3)
                m = jnp.concatenate([m[:, :, h : h + 1] for h in range(ny // 8)[::-1]], axis=2)
                m = m.reshape(2, comps, ny, nz)
                e = (p + m).astype(bf16)
                er, ei = e[0], e[1]
                oi = (p[1] - m[1]).astype(bf16)
                minus_or = (m[0] - p[0]).astype(bf16)
            else:
                x = (half if xl == 0 else gx - XB + xl) if chunk == folded else xl
                p = pv[:, :, x]
                er, ei, oi, minus_or = p[0], p[1], p[1], -p[0]
            wr[slot, :, pl.ds(k, ny), :] = er
            wi[slot, :, pl.ds(k, ny), :] = ei
            wr[slot, :, pl.ds(kb + k, ny), :] = oi
            wi[slot, :, pl.ds(kb + k, ny), :] = minus_or

    def multiply(slot, depth, block):
        a, b = 2 * block, 2 * block + 1
        w = jnp.concatenate([x[slot, i, :depth] for x in (wr, wi) for i in (a, b)], axis=1)
        return lax.dot_general(
            w, t_ref[slot, :depth], (((0,), (0,)), ((), ())), preferred_element_type=f32
        )

    firsts = [sum(GROUPS[:i]) for i in range(len(GROUPS))]

    def prepare(step):
        for n in range(GROUPS[step]):
            chunk = firsts[step] + n
            for cp in copies[chunk]:
                cp.wait()
            if chunk + AHEAD < chunks:
                for cp in copies[chunk + AHEAD]:
                    cp.start()
        for n in range(GROUPS[step]):
            chunk = firsts[step] + n
            make_tables(chunk, step % 2, 2 * kb * n)
            fill(chunk, step % 2, 2 * kb * n)

    blocks = comps // 2
    rows = 4 * nz
    prepare(0)
    for step in range(len(GROUPS)):
        depth = 2 * kb * GROUPS[step]
        last = step == len(GROUPS) - 1
        for block in range(blocks):
            g = multiply(step % 2, depth, block)
            window = pl.ds(block * rows, rows)
            if step > 0:
                g = acc_ref[window, :] + g
            if not last:
                acc_ref[window, :] = g
                if block == 0:
                    prepare(step + 1)
                    if step == 0:
                        z_phases()
            else:
                for i in range(2):
                    re = g[i * nz : (i + 1) * nz]
                    im = g[(2 + i) * nz : (3 + i) * nz]
                    cz, sz = cz_ref[...], sz_ref[...]
                    comp = 2 * block + i
                    out_ref[comp : comp + 1, :] = jnp.sum(re * cz + im * sz, axis=0, keepdims=True)
                    out_ref[comps + comp : comps + comp + 1, :] = jnp.sum(im * cz - re * sz, axis=0, keepdims=True)


def far_field(p, th, ph):
    dirs = th.shape[0]
    r, comps, gx, ny, nz = p.shape
    depth = 2 * XB * ny * max(GROUPS)
    rows = gx // 2 + 8
    hbm = pl.BlockSpec(memory_space=pltpu.HBM)
    vmem = pl.BlockSpec(memory_space=pltpu.VMEM)
    return pl.pallas_call(
        far_field_kernel,
        name="far_field",
        out_shape=(
            jax.ShapeDtypeStruct((2 * comps, dirs), jnp.float32),
            jax.ShapeDtypeStruct((4, dirs), jnp.float32),
        ),
        in_specs=[hbm, hbm, hbm],
        out_specs=(vmem, vmem),
        scratch_shapes=[
            pltpu.VMEM((dirs,), jnp.int32),
            pltpu.VMEM((dirs,), jnp.int32),
            pltpu.VMEM((r, comps, gx, ny, nz), jnp.bfloat16),
            pltpu.VMEM((2, comps, depth, nz), jnp.bfloat16),
            pltpu.VMEM((2, comps, depth, nz), jnp.bfloat16),
            pltpu.VMEM((2, depth, dirs), jnp.bfloat16),
            pltpu.VMEM((2 * comps * nz, dirs), jnp.float32),
            pltpu.VMEM((rows, dirs), jnp.float32),
            pltpu.VMEM((rows, dirs), jnp.float32),
            pltpu.VMEM((nz, dirs), jnp.float32),
            pltpu.VMEM((nz, dirs), jnp.float32),
            pltpu.SemaphoreType.DMA((2,)),
            pltpu.SemaphoreType.DMA((2 * (gx // 2 // XB) + 1,)),
        ],
        compiler_params=pltpu.CompilerParams(vmem_limit_bytes=52 * 2**20),
    )(th, ph, p)


PAULI = (((1, 0), (0, 1)), ((1, 0), (0, -1)), ((0, 1), (1, 0)), ((0, -1j), (1j, 0)))


def mueller_kernel(x_ref, m2_ref, m1_ref, mw_ref, unit_ref, o_ref):
    amplitude = (x_ref[...] + m2_ref[...]) + (m1_ref[...] + mw_ref[...])
    ct, st, cp, sp = (unit_ref[i : i + 1, :] for i in range(4))
    units = ((ct * cp, ct * sp, -st), (-sp, cp))
    re = [[None, None], [None, None]]
    im = [[None, None], [None, None]]
    for s, unit in enumerate(units):
        for p in range(2):
            a = b = 0.0
            for c, u in enumerate(unit):
                a = a + u * amplitude[3 * p + c : 3 * p + c + 1]
                b = b + u * amplitude[6 + 3 * p + c : 7 + 3 * p + c]
            re[s][p], im[s][p] = a, b
    known = {}

    def product(b, c, a, e):
        if (b, c, a, e) not in known:
            known[b, c, a, e] = (
                re[b][c] * re[a][e] + im[b][c] * im[a][e],
                im[b][c] * re[a][e] - re[b][c] * im[a][e],
            )
        return known[b, c, a, e]

    for i in range(4):
        for j in range(4):
            total = 0.0
            for a in range(2):
                for b in range(2):
                    for c in range(2):
                        for e in range(2):
                            weight = complex(PAULI[i][a][b]) * complex(PAULI[j][c][e])
                            if weight == 0:
                                continue
                            zr, zi = product(b, c, a, e)
                            if weight.real:
                                total = total + weight.real * zr
                            if weight.imag:
                                total = total - weight.imag * zi
            o_ref[4 * i + j : 4 * i + j + 1, :] = 0.5 * total


def mueller(parts, units):
    return pl.pallas_call(
        mueller_kernel,
        name="mueller",
        out_shape=jax.ShapeDtypeStruct((16, units.shape[1]), jnp.float32),
    )(*parts, units)


NEAR, WRAP, FAR = (1, 0, 3, 2), (3, 2, 1, 0), (2, 3, 0, 1)


def ring_partners(x, axis, inner):
    size = lax.axis_size(axis)

    def moved(pairing):
        def partner(i):
            at = i // inner % 4
            return i + (pairing[at] - at) * inner

        return lax.ppermute(x, axis, [(i, partner(i)) for i in range(size)])

    near, wrap, far = moved(NEAR), moved(WRAP), moved(FAR)
    return x, far, near, wrap


def ring_sum(x, axis, inner):
    own, far, near, wrap = ring_partners(x, axis, inner)
    return (own + far) + (near + wrap)


def body(polarization, theta_index, phi_index):
    x, units = far_field(polarization, theta_index, phi_index)
    x = x + lax.ppermute(x, "zs", [(i, i ^ 1) for i in range(lax.axis_size("zs"))])
    x = ring_sum(x, "zs", 2)
    x = ring_sum(x, "ys", 1)
    return mueller(ring_partners(x, "ys", 4), units)


def solution(mesh):
    return jax.shard_map(
        body,
        mesh=mesh,
        in_specs=(P(None, None, None, "ys", "zs"), P(), P()),
        out_specs=P(),
        check_vma=False,
    )
```

```python
import math

import jax
import jax.numpy as jnp
from jax import lax
from jax.experimental import pallas as pl
from jax.experimental.pallas import tpu as pltpu
from jax.sharding import PartitionSpec as P

WAVE = 0.6
NTHETA = 180
NPHI = 360
XB = 16
GROUPS = (1, 2, 3, 3)
AHEAD = 9


def sincos_turns(u):
    r = u - jnp.floor(u + 0.5)
    t = r * r
    w = 2.0 * math.pi
    cos_k = [(-1) ** n * w ** (2 * n) / math.factorial(2 * n) for n in range(11)]
    sin_k = [(-1) ** n * w ** (2 * n + 1) / math.factorial(2 * n + 1) for n in range(10)]
    c = jnp.full_like(t, cos_k[-1])
    for k in cos_k[-2::-1]:
        c = c * t + k
    s = jnp.full_like(t, sin_k[-1])
    for k in sin_k[-2::-1]:
        s = s * t + k
    return c, s * r


def far_field_kernel(
    idx_ref, p_hbm, out_ref, unit_ref,
    pv, wr, wi, t_ref, acc_ref, tc_ref, ts_ref, cz_ref, sz_ref, mirror, sems,
):
    _, comps, gx, ny, nz = pv.shape
    half = gx // 2
    dirs = out_ref.shape[1]
    f32, bf16 = jnp.float32, jnp.bfloat16
    folded = half // XB - 1
    kb = XB * ny

    pieces = [[(0, XB)], [(half, 1), (gx - XB + 1, XB - 1)]]
    pieces += [[(half + 1 + XB * i, XB), (half - XB * (i + 1), XB)] for i in range(folded)]
    copies = []
    count = 0
    for group in pieces:
        made = []
        for x0, length in group:
            window = pl.ds(x0, length)
            made.append(pltpu.make_async_copy(p_hbm.at[:, :, window], pv.at[:, :, window], sems.at[count]))
            count += 1
        copies.append(made)
    chunks = len(copies)
    for made in copies[:AHEAD]:
        for cp in made:
            cp.start()

    ct, st = sincos_turns((idx_ref[0:1, :].astype(f32) + 0.5) * (0.5 / NTHETA))
    cp_, sp_ = sincos_turns(idx_ref[1:2, :].astype(f32) * (1.0 / NPHI))
    unit_ref[...] = jnp.concatenate([ct, st, cp_, sp_], axis=0)
    scale = WAVE / (2.0 * math.pi)
    ux, uy, uz = scale * (st * cp_), scale * (st * sp_), scale * ct
    inner = lax.broadcasted_iota(jnp.int32, (16, dirs), 0).astype(f32)
    outer = lax.broadcasted_iota(jnp.int32, (8, dirs), 0).astype(f32) * 16.0

    def rotated(cos_in, sin_in, cos_out, sin_out, i):
        c, s = cos_out[i : i + 1], sin_out[i : i + 1]
        return cos_in * c - sin_in * s, sin_in * c + cos_in * s

    tc_ref[0:8, :] = jnp.ones((8, dirs), f32)
    ts_ref[0:8, :] = jnp.zeros((8, dirs), f32)
    x_in, x_out = sincos_turns((inner + 1.0) * ux), sincos_turns(outer * ux)
    for i in range(half // 16):
        c, s = rotated(*x_in, *x_out, i)
        tc_ref[8 + 16 * i : 24 + 16 * i, :] = c.astype(bf16).astype(f32)
        ts_ref[8 + 16 * i : 24 + 16 * i, :] = s.astype(bf16).astype(f32)
    qy = lax.broadcasted_iota(jnp.int32, (ny, dirs), 0).astype(f32) - (ny - 1) / 2.0
    cy, sy = sincos_turns(qy * uy)
    flip = 7 - lax.broadcasted_iota(jnp.int32, (2, comps, ny // 8, 8, nz), 3)

    def z_phases():
        ys, total_y = lax.axis_index("ys"), ny * lax.axis_size("ys")
        zs, total_z = lax.axis_index("zs"), nz * lax.axis_size("zs")
        y_mid = (ys * ny - total_y // 2).astype(f32) + (ny - 1) / 2.0
        z_first = (zs * nz - total_z // 2).astype(f32)
        total = 1.0 / math.sqrt(gx * total_y * total_z)
        c, s = sincos_turns((inner + z_first) * uz + y_mid * uy)
        z_in, z_out = (c * total, s * total), sincos_turns(outer * uz)
        for i in range(nz // 16):
            c, s = rotated(*z_in, *z_out, i)
            cz_ref[16 * i : 16 * i + 16, :] = c
            sz_ref[16 * i : 16 * i + 16, :] = s

    def make_tables(chunk, slot, k0):
        for xl in range(XB):
            if chunk == 0:
                px = xl - half
            elif chunk == 1:
                px = 0 if xl == 0 else half - XB + xl
            else:
                px = 1 + XB * (chunk - 2) + xl
            row = abs(px) + 7 if px else 0
            tc = tc_ref[pl.ds(row, 1), :]
            ts = ts_ref[pl.ds(row, 1), :]
            if px < 0:
                ts = -ts
            k = k0 + xl * ny
            t_ref[slot, pl.ds(k, ny), :] = (tc * cy - ts * sy).astype(bf16)
            t_ref[slot, pl.ds(kb + k, ny), :] = (ts * cy + tc * sy).astype(bf16)

    def fill(chunk, slot, k0):
        for xl in range(XB):
            k = k0 + xl * ny
            if chunk >= 2:
                off = 1 + XB * (chunk - 2) + xl
                p = pv[:, :, half + off]
                m = pv[:, :, half - off].astype(f32).reshape(2, comps, ny // 8, 8, nz)
                m = jnp.take_along_axis(m, flip, axis=3)
                m = jnp.concatenate([m[:, :, h : h + 1] for h in range(ny // 8)[::-1]], axis=2)
                mirror[off % 2] = m.reshape(2, comps, ny, nz).astype(bf16)
                m = mirror[off % 2]
                er, ei, oi, minus_or = p[0] + m[0], p[1] + m[1], p[1] - m[1], m[0] - p[0]
            else:
                x = (half if xl == 0 else gx - XB + xl) if chunk else xl
                p = pv[:, :, x]
                er, ei, oi, minus_or = p[0], p[1], p[1], -p[0]
            wr[slot, :, pl.ds(k, ny), :] = er
            wi[slot, :, pl.ds(k, ny), :] = ei
            wr[slot, :, pl.ds(kb + k, ny), :] = oi
            wi[slot, :, pl.ds(kb + k, ny), :] = minus_or

    def multiply(slot, depth, block):
        a, b = 2 * block, 2 * block + 1
        w = jnp.concatenate([x[slot, i, :depth] for x in (wr, wi) for i in (a, b)], axis=1)
        return lax.dot_general(
            w, t_ref[slot, :depth], (((0,), (0,)), ((), ())), preferred_element_type=f32
        )

    firsts = [sum(GROUPS[:i]) for i in range(len(GROUPS))]

    def prepare(step):
        for n in range(GROUPS[step]):
            chunk = firsts[step] + n
            for cp in copies[chunk]:
                cp.wait()
            if chunk + AHEAD < chunks:
                for cp in copies[chunk + AHEAD]:
                    cp.start()
        for n in range(GROUPS[step]):
            chunk = firsts[step] + n
            make_tables(chunk, step % 2, 2 * kb * n)
            fill(chunk, step % 2, 2 * kb * n)

    blocks = comps // 2
    rows = 4 * nz
    prepare(0)
    for step in range(len(GROUPS)):
        depth = 2 * kb * GROUPS[step]
        last = step == len(GROUPS) - 1
        for block in range(blocks):
            g = multiply(step % 2, depth, block)
            window = pl.ds(block * rows, rows)
            if step > 0:
                g = acc_ref[window, :] + g
            if not last:
                acc_ref[window, :] = g
                if block == 0:
                    prepare(step + 1)
                    if step == 0:
                        z_phases()
            else:
                for i in range(2):
                    re = g[i * nz : (i + 1) * nz]
                    im = g[(2 + i) * nz : (3 + i) * nz]
                    cz, sz = cz_ref[...], sz_ref[...]
                    comp = 2 * block + i
                    out_ref[comp : comp + 1, :] = jnp.sum(re * cz + im * sz, axis=0, keepdims=True)
                    out_ref[comps + comp : comps + comp + 1, :] = jnp.sum(im * cz - re * sz, axis=0, keepdims=True)


def far_field(p, th, ph):
    dirs = th.shape[0]
    idx = jnp.stack([th, ph])
    r, comps, gx, ny, nz = p.shape
    depth = 2 * XB * ny * max(GROUPS)
    rows = gx // 2 + 8
    hbm = pl.BlockSpec(memory_space=pltpu.HBM)
    vmem = pl.BlockSpec(memory_space=pltpu.VMEM)
    return pl.pallas_call(
        far_field_kernel,
        name="far_field",
        out_shape=(
            jax.ShapeDtypeStruct((2 * comps, dirs), jnp.float32),
            jax.ShapeDtypeStruct((4, dirs), jnp.float32),
        ),
        in_specs=[vmem, hbm],
        out_specs=(vmem, vmem),
        scratch_shapes=[
            pltpu.VMEM((r, comps, gx, ny, nz), jnp.bfloat16),
            pltpu.VMEM((2, comps, depth, nz), jnp.bfloat16),
            pltpu.VMEM((2, comps, depth, nz), jnp.bfloat16),
            pltpu.VMEM((2, depth, dirs), jnp.bfloat16),
            pltpu.VMEM((2 * comps * nz, dirs), jnp.float32),
            pltpu.VMEM((rows, dirs), jnp.float32),
            pltpu.VMEM((rows, dirs), jnp.float32),
            pltpu.VMEM((nz, dirs), jnp.float32),
            pltpu.VMEM((nz, dirs), jnp.float32),
            pltpu.VMEM((2, r, comps, ny, nz), jnp.bfloat16),
            pltpu.SemaphoreType.DMA((2 * (gx // 2 // XB) + 1,)),
        ],
        compiler_params=pltpu.CompilerParams(vmem_limit_bytes=52 * 2**20),
    )(idx, p)


PAULI = (((1, 0), (0, 1)), ((1, 0), (0, -1)), ((0, 1), (1, 0)), ((0, -1j), (1j, 0)))


def mueller_kernel(x_ref, m2_ref, m1_ref, mw_ref, unit_ref, o_ref):
    amplitude = (x_ref[...] + m2_ref[...]) + (m1_ref[...] + mw_ref[...])
    ct, st, cp, sp = (unit_ref[i : i + 1, :] for i in range(4))
    units = ((ct * cp, ct * sp, -st), (-sp, cp))
    re = [[None, None], [None, None]]
    im = [[None, None], [None, None]]
    for s, unit in enumerate(units):
        for p in range(2):
            a = b = 0.0
            for c, u in enumerate(unit):
                a = a + u * amplitude[3 * p + c : 3 * p + c + 1]
                b = b + u * amplitude[6 + 3 * p + c : 7 + 3 * p + c]
            re[s][p], im[s][p] = a, b
    known = {}

    def product(b, c, a, e):
        if (b, c, a, e) not in known:
            known[b, c, a, e] = (
                re[b][c] * re[a][e] + im[b][c] * im[a][e],
                im[b][c] * re[a][e] - re[b][c] * im[a][e],
            )
        return known[b, c, a, e]

    for i in range(4):
        for j in range(4):
            total = 0.0
            for a in range(2):
                for b in range(2):
                    for c in range(2):
                        for e in range(2):
                            weight = complex(PAULI[i][a][b]) * complex(PAULI[j][c][e])
                            if weight == 0:
                                continue
                            zr, zi = product(b, c, a, e)
                            if weight.real:
                                total = total + weight.real * zr
                            if weight.imag:
                                total = total - weight.imag * zi
            o_ref[4 * i + j : 4 * i + j + 1, :] = 0.5 * total


def mueller(parts, units):
    return pl.pallas_call(
        mueller_kernel,
        name="mueller",
        out_shape=jax.ShapeDtypeStruct((16, units.shape[1]), jnp.float32),
        in_specs=[pl.BlockSpec(memory_space=pltpu.VMEM)] * 5,
        out_specs=pl.BlockSpec(memory_space=pltpu.VMEM),
        compiler_params=pltpu.CompilerParams(vmem_limit_bytes=4 * 2**20),
    )(*parts, units)


NEAR, WRAP, FAR = (1, 0, 3, 2), (3, 2, 1, 0), (2, 3, 0, 1)


def ring_partners(x, axis, inner):
    size = lax.axis_size(axis)

    def moved(pairing):
        def partner(i):
            at = i // inner % 4
            return i + (pairing[at] - at) * inner

        return lax.ppermute(x, axis, [(i, partner(i)) for i in range(size)])

    near, wrap, far = moved(NEAR), moved(WRAP), moved(FAR)
    return x, far, near, wrap


def ring_sum(x, axis, inner):
    own, far, near, wrap = ring_partners(x, axis, inner)
    return (own + far) + (near + wrap)


def body(polarization, theta_index, phi_index):
    x, units = far_field(polarization, theta_index, phi_index)
    x = x + lax.ppermute(x, "zs", [(i, i ^ 1) for i in range(lax.axis_size("zs"))])
    x = ring_sum(x, "zs", 2)
    x = ring_sum(x, "ys", 1)
    return mueller(ring_partners(x, "ys", 4), units)


def solution(mesh):
    return jax.shard_map(
        body,
        mesh=mesh,
        in_specs=(P(None, None, None, "ys", "zs"), P(), P()),
        out_specs=P(),
        check_vma=False,
    )
```

```python
import math

import jax
import jax.numpy as jnp
from jax import lax
from jax.experimental import pallas as pl
from jax.experimental.pallas import tpu as pltpu
from jax.sharding import PartitionSpec as P

WAVE = 0.6
NTHETA = 180
NPHI = 360
XB = 16
GROUPS = (1, 2, 3, 3)
AHEAD = 9


def sincos_turns(u):
    r = u - jnp.floor(u + 0.5)
    t = r * r
    w = 2.0 * math.pi
    cos_k = [(-1) ** n * w ** (2 * n) / math.factorial(2 * n) for n in range(11)]
    sin_k = [(-1) ** n * w ** (2 * n + 1) / math.factorial(2 * n + 1) for n in range(10)]
    c = jnp.full_like(t, cos_k[-1])
    for k in cos_k[-2::-1]:
        c = c * t + k
    s = jnp.full_like(t, sin_k[-1])
    for k in sin_k[-2::-1]:
        s = s * t + k
    return c, s * r


def far_field_kernel(
    idx_ref, p_hbm, out_ref, unit_ref,
    pv, wr, wi, t_ref, acc_ref, tc_ref, ts_ref, cz_ref, sz_ref, sems,
):
    _, comps, gx, ny, nz = pv.shape
    half = gx // 2
    dirs = out_ref.shape[1]
    f32, bf16 = jnp.float32, jnp.bfloat16
    folded = half // XB - 1
    kb = XB * ny

    pieces = [[(0, XB)], [(half, 1), (gx - XB + 1, XB - 1)]]
    pieces += [[(half + 1 + XB * i, XB), (half - XB * (i + 1), XB)] for i in range(folded)]
    copies = []
    count = 0
    for group in pieces:
        made = []
        for x0, length in group:
            window = pl.ds(x0, length)
            made.append(pltpu.make_async_copy(p_hbm.at[:, :, window], pv.at[:, :, window], sems.at[count]))
            count += 1
        copies.append(made)
    chunks = len(copies)
    for made in copies[:AHEAD]:
        for cp in made:
            cp.start()

    ct, st = sincos_turns((idx_ref[0:1, :].astype(f32) + 0.5) * (0.5 / NTHETA))
    cp_, sp_ = sincos_turns(idx_ref[1:2, :].astype(f32) * (1.0 / NPHI))
    unit_ref[...] = jnp.concatenate([ct, st, cp_, sp_], axis=0)
    scale = WAVE / (2.0 * math.pi)
    ux, uy, uz = scale * (st * cp_), scale * (st * sp_), scale * ct
    inner = lax.broadcasted_iota(jnp.int32, (16, dirs), 0).astype(f32)
    outer = lax.broadcasted_iota(jnp.int32, (8, dirs), 0).astype(f32) * 16.0

    def rotated(cos_in, sin_in, cos_out, sin_out, i):
        c, s = cos_out[i : i + 1], sin_out[i : i + 1]
        return cos_in * c - sin_in * s, sin_in * c + cos_in * s

    tc_ref[0:8, :] = jnp.ones((8, dirs), f32)
    ts_ref[0:8, :] = jnp.zeros((8, dirs), f32)
    x_in, x_out = sincos_turns((inner + 1.0) * ux), sincos_turns(outer * ux)
    for i in range(half // 16):
        c, s = rotated(*x_in, *x_out, i)
        tc_ref[8 + 16 * i : 24 + 16 * i, :] = c.astype(bf16).astype(f32)
        ts_ref[8 + 16 * i : 24 + 16 * i, :] = s.astype(bf16).astype(f32)
    qy = lax.broadcasted_iota(jnp.int32, (ny, dirs), 0).astype(f32) - (ny - 1) / 2.0
    cy, sy = sincos_turns(qy * uy)
    flip = 7 - lax.broadcasted_iota(jnp.int32, (2, comps, ny // 8, 8, nz), 3)

    def z_phases():
        ys, total_y = lax.axis_index("ys"), ny * lax.axis_size("ys")
        zs, total_z = lax.axis_index("zs"), nz * lax.axis_size("zs")
        y_mid = (ys * ny - total_y // 2).astype(f32) + (ny - 1) / 2.0
        z_first = (zs * nz - total_z // 2).astype(f32)
        total = 1.0 / math.sqrt(gx * total_y * total_z)
        c, s = sincos_turns((inner + z_first) * uz + y_mid * uy)
        z_in, z_out = (c * total, s * total), sincos_turns(outer * uz)
        for i in range(nz // 16):
            c, s = rotated(*z_in, *z_out, i)
            cz_ref[16 * i : 16 * i + 16, :] = c
            sz_ref[16 * i : 16 * i + 16, :] = s

    def make_tables(chunk, slot, k0):
        for xl in range(XB):
            if chunk == 0:
                px = xl - half
            elif chunk == 1:
                px = 0 if xl == 0 else half - XB + xl
            else:
                px = 1 + XB * (chunk - 2) + xl
            row = abs(px) + 7 if px else 0
            tc = tc_ref[pl.ds(row, 1), :]
            ts = ts_ref[pl.ds(row, 1), :]
            if px < 0:
                ts = -ts
            k = k0 + xl * ny
            t_ref[slot, pl.ds(k, ny), :] = (tc * cy - ts * sy).astype(bf16)
            t_ref[slot, pl.ds(kb + k, ny), :] = (ts * cy + tc * sy).astype(bf16)

    def fill(chunk, slot, k0):
        for xl in range(XB):
            k = k0 + xl * ny
            if chunk >= 2:
                off = 1 + XB * (chunk - 2) + xl
                p = pv[:, :, half + off].astype(f32)
                m = pv[:, :, half - off].astype(f32).reshape(2, comps, ny // 8, 8, nz)
                m = jnp.take_along_axis(m, flip, axis=3)
                m = jnp.concatenate([m[:, :, h : h + 1] for h in range(ny // 8)[::-1]], axis=2)
                m = m.reshape(2, comps, ny, nz)
                e = (p + m).astype(bf16)
                er, ei = e[0], e[1]
                oi = (p[1] - m[1]).astype(bf16)
                minus_or = (m[0] - p[0]).astype(bf16)
            else:
                x = (half if xl == 0 else gx - XB + xl) if chunk else xl
                p = pv[:, :, x]
                er, ei, oi, minus_or = p[0], p[1], p[1], -p[0]
            wr[slot, :, pl.ds(k, ny), :] = er
            wi[slot, :, pl.ds(k, ny), :] = ei
            wr[slot, :, pl.ds(kb + k, ny), :] = oi
            wi[slot, :, pl.ds(kb + k, ny), :] = minus_or

    def multiply(slot, depth, block):
        a, b = 2 * block, 2 * block + 1
        w = jnp.concatenate([x[slot, i, :depth] for x in (wr, wi) for i in (a, b)], axis=1)
        return lax.dot_general(
            w, t_ref[slot, :depth], (((0,), (0,)), ((), ())), preferred_element_type=f32
        )

    firsts = [sum(GROUPS[:i]) for i in range(len(GROUPS))]

    def prepare(step):
        for n in range(GROUPS[step]):
            chunk = firsts[step] + n
            for cp in copies[chunk]:
                cp.wait()
            if chunk + AHEAD < chunks:
                for cp in copies[chunk + AHEAD]:
                    cp.start()
        for n in range(GROUPS[step]):
            chunk = firsts[step] + n
            make_tables(chunk, step % 2, 2 * kb * n)
            fill(chunk, step % 2, 2 * kb * n)

    blocks = comps // 2
    rows = 4 * nz
    prepare(0)
    for step in range(len(GROUPS)):
        depth = 2 * kb * GROUPS[step]
        last = step == len(GROUPS) - 1
        for block in range(blocks):
            g = multiply(step % 2, depth, block)
            window = pl.ds(block * rows, rows)
            if step > 0:
                g = acc_ref[window, :] + g
            if not last:
                acc_ref[window, :] = g
                if block == 0:
                    prepare(step + 1)
                    if step == 0:
                        z_phases()
            else:
                for i in range(2):
                    re = g[i * nz : (i + 1) * nz]
                    im = g[(2 + i) * nz : (3 + i) * nz]
                    cz, sz = cz_ref[...], sz_ref[...]
                    comp = 2 * block + i
                    out_ref[comp : comp + 1, :] = jnp.sum(re * cz + im * sz, axis=0, keepdims=True)
                    out_ref[comps + comp : comps + comp + 1, :] = jnp.sum(im * cz - re * sz, axis=0, keepdims=True)


def far_field(p, th, ph):
    dirs = th.shape[0]
    idx = jnp.stack([th, ph])
    r, comps, gx, ny, nz = p.shape
    depth = 2 * XB * ny * max(GROUPS)
    rows = gx // 2 + 8
    hbm = pl.BlockSpec(memory_space=pltpu.HBM)
    vmem = pl.BlockSpec(memory_space=pltpu.VMEM)
    return pl.pallas_call(
        far_field_kernel,
        name="far_field",
        out_shape=(
            jax.ShapeDtypeStruct((2 * comps, dirs), jnp.float32),
            jax.ShapeDtypeStruct((4, dirs), jnp.float32),
        ),
        in_specs=[vmem, hbm],
        out_specs=(vmem, vmem),
        scratch_shapes=[
            pltpu.VMEM((r, comps, gx, ny, nz), jnp.bfloat16),
            pltpu.VMEM((2, comps, depth, nz), jnp.bfloat16),
            pltpu.VMEM((2, comps, depth, nz), jnp.bfloat16),
            pltpu.VMEM((2, depth, dirs), jnp.bfloat16),
            pltpu.VMEM((2 * comps * nz, dirs), jnp.float32),
            pltpu.VMEM((rows, dirs), jnp.float32),
            pltpu.VMEM((rows, dirs), jnp.float32),
            pltpu.VMEM((nz, dirs), jnp.float32),
            pltpu.VMEM((nz, dirs), jnp.float32),
            pltpu.SemaphoreType.DMA((2 * (gx // 2 // XB) + 1,)),
        ],
        compiler_params=pltpu.CompilerParams(vmem_limit_bytes=52 * 2**20),
    )(idx, p)


PAULI = (((1, 0), (0, 1)), ((1, 0), (0, -1)), ((0, 1), (1, 0)), ((0, -1j), (1j, 0)))


def mueller_kernel(x_ref, m2_ref, m1_ref, mw_ref, unit_ref, o_ref):
    amplitude = (x_ref[...] + m2_ref[...]) + (m1_ref[...] + mw_ref[...])
    ct, st, cp, sp = (unit_ref[i : i + 1, :] for i in range(4))
    units = ((ct * cp, ct * sp, -st), (-sp, cp))
    re = [[None, None], [None, None]]
    im = [[None, None], [None, None]]
    for s, unit in enumerate(units):
        for p in range(2):
            a = b = 0.0
            for c, u in enumerate(unit):
                a = a + u * amplitude[3 * p + c : 3 * p + c + 1]
                b = b + u * amplitude[6 + 3 * p + c : 7 + 3 * p + c]
            re[s][p], im[s][p] = a, b
    known = {}

    def product(b, c, a, e):
        if (b, c, a, e) not in known:
            known[b, c, a, e] = (
                re[b][c] * re[a][e] + im[b][c] * im[a][e],
                im[b][c] * re[a][e] - re[b][c] * im[a][e],
            )
        return known[b, c, a, e]

    for i in range(4):
        for j in range(4):
            total = 0.0
            for a in range(2):
                for b in range(2):
                    for c in range(2):
                        for e in range(2):
                            weight = complex(PAULI[i][a][b]) * complex(PAULI[j][c][e])
                            if weight == 0:
                                continue
                            zr, zi = product(b, c, a, e)
                            if weight.real:
                                total = total + weight.real * zr
                            if weight.imag:
                                total = total - weight.imag * zi
            o_ref[4 * i + j : 4 * i + j + 1, :] = 0.5 * total


def mueller(parts, units):
    return pl.pallas_call(
        mueller_kernel,
        name="mueller",
        out_shape=jax.ShapeDtypeStruct((16, units.shape[1]), jnp.float32),
        in_specs=[pl.BlockSpec(memory_space=pltpu.VMEM)] * 5,
        out_specs=pl.BlockSpec(memory_space=pltpu.VMEM),
        compiler_params=pltpu.CompilerParams(vmem_limit_bytes=4 * 2**20),
    )(*parts, units)


NEAR, WRAP, FAR = (1, 0, 3, 2), (3, 2, 1, 0), (2, 3, 0, 1)


def ring_partners(x, axis, inner):
    size = lax.axis_size(axis)

    def moved(pairing):
        def partner(i):
            at = i // inner % 4
            return i + (pairing[at] - at) * inner

        return lax.ppermute(x, axis, [(i, partner(i)) for i in range(size)])

    near, wrap, far = moved(NEAR), moved(WRAP), moved(FAR)
    return x, far, near, wrap


def ring_sum(x, axis, inner):
    own, far, near, wrap = ring_partners(x, axis, inner)
    return (own + far) + (near + wrap)


def body(polarization, theta_index, phi_index):
    x, units = far_field(polarization, theta_index, phi_index)
    x = x + lax.ppermute(x, "zs", [(i, i ^ 1) for i in range(lax.axis_size("zs"))])
    x = ring_sum(x, "zs", 2)
    x = ring_sum(x, "ys", 1)
    return mueller(ring_partners(x, "ys", 4), units)


def solution(mesh):
    return jax.shard_map(
        body,
        mesh=mesh,
        in_specs=(P(None, None, None, "ys", "zs"), P(), P()),
        out_specs=P(),
        check_vma=False,
    )
```

```python
import math

import jax
import jax.numpy as jnp
from jax import lax
from jax.experimental import pallas as pl
from jax.experimental.pallas import tpu as pltpu
from jax.sharding import PartitionSpec as P

WAVE = 0.6
NTHETA = 180
NPHI = 360
XB = 16
GROUPS = (1, 2, 3, 3)


def sincos_turns(u):
    r = u - jnp.floor(u + 0.5)
    t = r * r
    w = 2.0 * math.pi
    cos_k = [(-1) ** n * w ** (2 * n) / math.factorial(2 * n) for n in range(11)]
    sin_k = [(-1) ** n * w ** (2 * n + 1) / math.factorial(2 * n + 1) for n in range(10)]
    c = jnp.full_like(t, cos_k[-1])
    for k in cos_k[-2::-1]:
        c = c * t + k
    s = jnp.full_like(t, sin_k[-1])
    for k in sin_k[-2::-1]:
        s = s * t + k
    return c, s * r


def far_field_kernel(
    th_hbm, ph_hbm, p_hbm, out_ref, unit_ref,
    th_ref, ph_ref, pv, wr, wi, t_ref, acc_ref, tc_ref, ts_ref, cz_ref, sz_ref, idx_sems, sems,
):
    _, comps, gx, ny, nz = pv.shape
    half = gx // 2
    dirs = out_ref.shape[1]
    f32, bf16 = jnp.float32, jnp.bfloat16
    folded = half // XB - 1
    kb = XB * ny

    idx_copies = [
        pltpu.make_async_copy(th_hbm, th_ref, idx_sems.at[0]),
        pltpu.make_async_copy(ph_hbm, ph_ref, idx_sems.at[1]),
    ]
    for cp in idx_copies:
        cp.start()
    pieces = [[(0, XB)], [(half, 1), (gx - XB + 1, XB - 1)]]
    pieces += [[(half + 1 + XB * i, XB), (half - XB * (i + 1), XB)] for i in range(folded)]
    copies = []
    count = 0
    for group in pieces:
        made = []
        for x0, length in group:
            window = pl.ds(x0, length)
            made.append(pltpu.make_async_copy(p_hbm.at[:, :, window], pv.at[:, :, window], sems.at[count]))
            count += 1
        copies.append(made)
    for cp in copies[0]:
        cp.start()

    for cp in idx_copies:
        cp.wait()
    for made in copies[1:]:
        for cp in made:
            cp.start()
    ct, st = sincos_turns((th_ref[...].reshape(1, dirs).astype(f32) + 0.5) * (0.5 / NTHETA))
    cp_, sp_ = sincos_turns(ph_ref[...].reshape(1, dirs).astype(f32) * (1.0 / NPHI))
    unit_ref[...] = jnp.concatenate([ct, st, cp_, sp_], axis=0)
    scale = WAVE / (2.0 * math.pi)
    ux, uy, uz = scale * (st * cp_), scale * (st * sp_), scale * ct
    inner = lax.broadcasted_iota(jnp.int32, (16, dirs), 0).astype(f32)
    outer = lax.broadcasted_iota(jnp.int32, (8, dirs), 0).astype(f32) * 16.0

    def rotated(cos_in, sin_in, cos_out, sin_out, i):
        c, s = cos_out[i : i + 1], sin_out[i : i + 1]
        return cos_in * c - sin_in * s, sin_in * c + cos_in * s

    tc_ref[0:8, :] = jnp.ones((8, dirs), f32)
    ts_ref[0:8, :] = jnp.zeros((8, dirs), f32)
    x_in, x_out = sincos_turns((inner + 1.0) * ux), sincos_turns(outer * ux)
    for i in range(half // 16):
        c, s = rotated(*x_in, *x_out, i)
        tc_ref[8 + 16 * i : 24 + 16 * i, :] = c.astype(bf16).astype(f32)
        ts_ref[8 + 16 * i : 24 + 16 * i, :] = s.astype(bf16).astype(f32)
    qy = lax.broadcasted_iota(jnp.int32, (ny, dirs), 0).astype(f32) - (ny - 1) / 2.0
    cy, sy = sincos_turns(qy * uy)
    flip = 7 - lax.broadcasted_iota(jnp.int32, (2, comps, ny // 8, 8, nz), 3)

    def z_phases():
        ys, total_y = lax.axis_index("ys"), ny * lax.axis_size("ys")
        zs, total_z = lax.axis_index("zs"), nz * lax.axis_size("zs")
        y_mid = (ys * ny - total_y // 2).astype(f32) + (ny - 1) / 2.0
        z_first = (zs * nz - total_z // 2).astype(f32)
        total = 1.0 / math.sqrt(gx * total_y * total_z)
        c, s = sincos_turns((inner + z_first) * uz + y_mid * uy)
        z_in, z_out = (c * total, s * total), sincos_turns(outer * uz)
        for i in range(nz // 16):
            c, s = rotated(*z_in, *z_out, i)
            cz_ref[16 * i : 16 * i + 16, :] = c
            sz_ref[16 * i : 16 * i + 16, :] = s

    def make_tables(chunk, slot, k0):
        for xl in range(XB):
            if chunk == 0:
                px = xl - half
            elif chunk == 1:
                px = 0 if xl == 0 else half - XB + xl
            else:
                px = 1 + XB * (chunk - 2) + xl
            row = abs(px) + 7 if px else 0
            tc = tc_ref[pl.ds(row, 1), :]
            ts = ts_ref[pl.ds(row, 1), :]
            if px < 0:
                ts = -ts
            k = k0 + xl * ny
            t_ref[slot, pl.ds(k, ny), :] = (tc * cy - ts * sy).astype(bf16)
            t_ref[slot, pl.ds(kb + k, ny), :] = (ts * cy + tc * sy).astype(bf16)

    def fill(chunk, slot, k0):
        for xl in range(XB):
            k = k0 + xl * ny
            if chunk >= 2:
                off = 1 + XB * (chunk - 2) + xl
                p = pv[:, :, half + off].astype(f32)
                m = pv[:, :, half - off].astype(f32).reshape(2, comps, ny // 8, 8, nz)
                m = jnp.take_along_axis(m, flip, axis=3)
                m = jnp.concatenate([m[:, :, h : h + 1] for h in range(ny // 8)[::-1]], axis=2)
                m = m.reshape(2, comps, ny, nz)
                e = (p + m).astype(bf16)
                er, ei = e[0], e[1]
                oi = (p[1] - m[1]).astype(bf16)
                minus_or = (m[0] - p[0]).astype(bf16)
            else:
                x = (half if xl == 0 else gx - XB + xl) if chunk else xl
                p = pv[:, :, x]
                er, ei, oi, minus_or = p[0], p[1], p[1], -p[0]
            wr[slot, :, pl.ds(k, ny), :] = er
            wi[slot, :, pl.ds(k, ny), :] = ei
            wr[slot, :, pl.ds(kb + k, ny), :] = oi
            wi[slot, :, pl.ds(kb + k, ny), :] = minus_or

    def multiply(slot, depth, block):
        a, b = 2 * block, 2 * block + 1
        w = jnp.concatenate([x[slot, i, :depth] for x in (wr, wi) for i in (a, b)], axis=1)
        return lax.dot_general(
            w, t_ref[slot, :depth], (((0,), (0,)), ((), ())), preferred_element_type=f32
        )

    firsts = [sum(GROUPS[:i]) for i in range(len(GROUPS))]

    def prepare(step):
        for n in range(GROUPS[step]):
            chunk = firsts[step] + n
            for cp in copies[chunk]:
                cp.wait()
        for n in range(GROUPS[step]):
            chunk = firsts[step] + n
            make_tables(chunk, step % 2, 2 * kb * n)
            fill(chunk, step % 2, 2 * kb * n)

    blocks = comps // 2
    rows = 4 * nz
    prepare(0)
    for step in range(len(GROUPS)):
        depth = 2 * kb * GROUPS[step]
        last = step == len(GROUPS) - 1
        for block in range(blocks):
            g = multiply(step % 2, depth, block)
            window = pl.ds(block * rows, rows)
            if step > 0:
                g = acc_ref[window, :] + g
            if not last:
                acc_ref[window, :] = g
                if block == 0:
                    prepare(step + 1)
                    if step == 0:
                        z_phases()
            else:
                for i in range(2):
                    re = g[i * nz : (i + 1) * nz]
                    im = g[(2 + i) * nz : (3 + i) * nz]
                    cz, sz = cz_ref[...], sz_ref[...]
                    comp = 2 * block + i
                    out_ref[comp : comp + 1, :] = jnp.sum(re * cz + im * sz, axis=0, keepdims=True)
                    out_ref[comps + comp : comps + comp + 1, :] = jnp.sum(im * cz - re * sz, axis=0, keepdims=True)


def far_field(p, th, ph):
    dirs = th.shape[0]
    th, ph = (pltpu.with_memory_space_constraint(i, pltpu.HBM) for i in (th, ph))
    r, comps, gx, ny, nz = p.shape
    depth = 2 * XB * ny * max(GROUPS)
    rows = gx // 2 + 8
    hbm = pl.BlockSpec(memory_space=pltpu.HBM)
    vmem = pl.BlockSpec(memory_space=pltpu.VMEM)
    return pl.pallas_call(
        far_field_kernel,
        name="far_field",
        out_shape=(
            jax.ShapeDtypeStruct((2 * comps, dirs), jnp.float32),
            jax.ShapeDtypeStruct((4, dirs), jnp.float32),
        ),
        in_specs=[hbm, hbm, hbm],
        out_specs=(vmem, vmem),
        scratch_shapes=[
            pltpu.VMEM((dirs,), jnp.int32),
            pltpu.VMEM((dirs,), jnp.int32),
            pltpu.VMEM((r, comps, gx, ny, nz), jnp.bfloat16),
            pltpu.VMEM((2, comps, depth, nz), jnp.bfloat16),
            pltpu.VMEM((2, comps, depth, nz), jnp.bfloat16),
            pltpu.VMEM((2, depth, dirs), jnp.bfloat16),
            pltpu.VMEM((2 * comps * nz, dirs), jnp.float32),
            pltpu.VMEM((rows, dirs), jnp.float32),
            pltpu.VMEM((rows, dirs), jnp.float32),
            pltpu.VMEM((nz, dirs), jnp.float32),
            pltpu.VMEM((nz, dirs), jnp.float32),
            pltpu.SemaphoreType.DMA((2,)),
            pltpu.SemaphoreType.DMA((2 * (gx // 2 // XB) + 1,)),
        ],
        compiler_params=pltpu.CompilerParams(vmem_limit_bytes=52 * 2**20),
    )(th, ph, p)


PAULI = (((1, 0), (0, 1)), ((1, 0), (0, -1)), ((0, 1), (1, 0)), ((0, -1j), (1j, 0)))


def mueller_kernel(x_ref, m2_ref, m1_ref, mw_ref, unit_ref, o_ref):
    amplitude = (x_ref[...] + m2_ref[...]) + (m1_ref[...] + mw_ref[...])
    ct, st, cp, sp = (unit_ref[i : i + 1, :] for i in range(4))
    units = ((ct * cp, ct * sp, -st), (-sp, cp))
    re = [[None, None], [None, None]]
    im = [[None, None], [None, None]]
    for s, unit in enumerate(units):
        for p in range(2):
            a = b = 0.0
            for c, u in enumerate(unit):
                a = a + u * amplitude[3 * p + c : 3 * p + c + 1]
                b = b + u * amplitude[6 + 3 * p + c : 7 + 3 * p + c]
            re[s][p], im[s][p] = a, b
    known = {}

    def product(b, c, a, e):
        if (b, c, a, e) not in known:
            known[b, c, a, e] = (
                re[b][c] * re[a][e] + im[b][c] * im[a][e],
                im[b][c] * re[a][e] - re[b][c] * im[a][e],
            )
        return known[b, c, a, e]

    for i in range(4):
        for j in range(4):
            total = 0.0
            for a in range(2):
                for b in range(2):
                    for c in range(2):
                        for e in range(2):
                            weight = complex(PAULI[i][a][b]) * complex(PAULI[j][c][e])
                            if weight == 0:
                                continue
                            zr, zi = product(b, c, a, e)
                            if weight.real:
                                total = total + weight.real * zr
                            if weight.imag:
                                total = total - weight.imag * zi
            o_ref[4 * i + j : 4 * i + j + 1, :] = 0.5 * total


def mueller(parts, units):
    return pl.pallas_call(
        mueller_kernel,
        name="mueller",
        out_shape=jax.ShapeDtypeStruct((16, units.shape[1]), jnp.float32),
        in_specs=[pl.BlockSpec(memory_space=pltpu.VMEM)] * 5,
        out_specs=pl.BlockSpec(memory_space=pltpu.VMEM),
        compiler_params=pltpu.CompilerParams(vmem_limit_bytes=4 * 2**20),
    )(*parts, units)


NEAR, WRAP, FAR = (1, 0, 3, 2), (3, 2, 1, 0), (2, 3, 0, 1)


def ring_partners(x, axis, inner):
    size = lax.axis_size(axis)

    def moved(pairing):
        def partner(i):
            at = i // inner % 4
            return i + (pairing[at] - at) * inner

        return lax.ppermute(x, axis, [(i, partner(i)) for i in range(size)])

    near, wrap, far = moved(NEAR), moved(WRAP), moved(FAR)
    return x, far, near, wrap


def ring_sum(x, axis, inner):
    own, far, near, wrap = ring_partners(x, axis, inner)
    return (own + far) + (near + wrap)


def body(polarization, theta_index, phi_index):
    x, units = far_field(polarization, theta_index, phi_index)
    x = x + lax.ppermute(x, "zs", [(i, i ^ 1) for i in range(lax.axis_size("zs"))])
    x = ring_sum(x, "zs", 2)
    x = ring_sum(x, "ys", 1)
    return mueller(ring_partners(x, "ys", 4), units)


def solution(mesh):
    return jax.shard_map(
        body,
        mesh=mesh,
        in_specs=(P(None, None, None, "ys", "zs"), P(), P()),
        out_specs=P(),
        check_vma=False,
    )
```
